32 devices in a mesh: dp: 8 (over z, x), tensor: 4 (over y, core).
Axes of the slice: x: 2, y: 2, z: 4, core: 2. Of those that a mesh axis runs over, the one named last changes fastest.
Arguments:
- streams: bfloat16 [128, 4, 7168], P('dp', None, 'tensor'), may hold values from -12 to 12
- mix_weight: bfloat16 [24, 4, 7168], P(None, None, 'tensor'), may hold values from -0.0625 to 0.0625
- mix_bias: float32 [24], replicated, may hold values from -4 to 4
- gate_weight: bfloat16 [18432, 7168], P('dp', 'tensor'), may hold values from -0.0625 to 0.0625
- up_weight: bfloat16 [18432, 7168], P('dp', 'tensor'), may hold values from -0.0625 to 0.0625
- down_weight: bfloat16 [18432, 7168], P('dp', 'tensor'), may hold values from -0.046875 to 0.046875
Outputs:
- new_streams: bfloat16 [128, 4, 7168], P('dp', None, 'tensor')
The draws below stay inside these ranges and needn't reach their ends.
All inputs are finite; a program needn't handle non-finite values.
Results may differ from the reference program's by a relative error of at most 0.006.
The reference program's roundings to bfloat16 on the way (of `mlp_input` and `hidden`) count: a program that leaves them out, or rounds other values in their place, can miss the bound.
Values may be sent and summed in bfloat16 or wider, within the bound.
No kernel may reach another device: no remote copies, remote signals or barrier semaphores. Data moves between devices by JAX's collectives and lax.ppermute only.
A program may use at most 64 MiB of HBM per device.

```python
import jax
import jax.numpy as jnp
from jax import lax

D = 7168
FF = 18432
STREAMS = 4
ITERS = 20
LOGITS = 24
TOKENS = 128


def draw_streams(key, part):
    normal_part = jax.random.normal(jax.random.fold_in(key, 11), (TOKENS, STREAMS, D), jnp.float32)
    return jnp.clip(normal_part, -12.0, 12.0).astype(jnp.bfloat16)


def block_scale(own_key, dims, split, low, high):
    level, own = 1.0, jax.random.fold_in(own_key, 6)
    for axis_at, shards_of in split:
        steps = jnp.exp(jax.random.uniform(jax.random.fold_in(own, axis_at), (shards_of,), jnp.float32, low / len(split), high / len(split)))
        level = level * jnp.repeat(steps, dims[axis_at] // shards_of).reshape([-1 if axis == axis_at else 1 for axis in range(len(dims))])
    return level


def gaussian(key, dims, width, limit, shards=(), held_as=jnp.bfloat16):
    entries = width * jax.random.normal(key, dims, jnp.float32)
    if shards:
        entries = entries * block_scale(key, dims, shards, -0.22, 0.18)
    return jnp.clip(entries, -limit, limit).astype(held_as)


def setup_inputs(seed: int = 0) -> dict:
    splits = jax.random.split(jax.random.key(seed), 7)
    streams = draw_streams(jax.random.fold_in(splits[6], 71), 0)
    mix_weight = gaussian(splits[1], (LOGITS, STREAMS, D), (2.0 / (STREAMS * D) ** 0.5), 0.0625, ((2, 4),))
    mix_bias = gaussian(splits[2], (LOGITS,), 1.0, 4.0, (), jnp.float32)
    gate_weight = gaussian(splits[3], (FF, D), D ** -0.5, 0.0625, ((0, 8), (1, 4)))
    up_weight = gaussian(splits[4], (FF, D), D ** -0.5, 0.0625, ((0, 8), (1, 4)))
    down_weight = gaussian(splits[5], (FF, D), FF ** -0.5, 0.046875, ((0, 8), (1, 4)))
    return {"streams": streams, "mix_weight": mix_weight, "mix_bias": mix_bias, "gate_weight": gate_weight, "up_weight": up_weight, "down_weight": down_weight}


epsilon = 1e-06

def normalize(sweep_index, matrix):
    matrix = matrix / lax.optimization_barrier(jnp.sum(matrix, axis=2, keepdims=True))
    return matrix / lax.optimization_barrier(jnp.sum(matrix, axis=1, keepdims=True))

def mixing(raw_logits, squares, mix_bias):
    scale_inv = lax.rsqrt(squares / (STREAMS * D) + epsilon)
    logits = raw_logits * scale_inv[:, None] + mix_bias[None, :]
    pre_gate = jax.nn.sigmoid(logits[:, :STREAMS])
    post_gate = 2.0 * jax.nn.sigmoid(logits[:, STREAMS:2 * STREAMS])
    matrix = jnp.exp(logits[:, 2 * STREAMS:]).reshape(-1, STREAMS, STREAMS)
    matrix = lax.fori_loop(0, ITERS, normalize, matrix)
    return (pre_gate, post_gate, matrix)

def reference(streams, mix_weight, mix_bias, gate_weight, up_weight, down_weight):
    row_count = streams.shape[0]
    flat_rows = streams.reshape(row_count, STREAMS * D)
    raw_logits = jnp.dot(flat_rows, mix_weight.reshape(LOGITS, STREAMS * D).T, preferred_element_type=jnp.float32)
    stream_wide = streams.astype(jnp.float32)
    squares = lax.optimization_barrier(jnp.sum(stream_wide * stream_wide, axis=(1, 2)))
    pre_gate, post_gate, res_mix = mixing(raw_logits, squares, mix_bias)
    mlp_input = jnp.einsum('ts,tsc->tc', pre_gate, stream_wide, precision=lax.Precision.HIGHEST).astype(jnp.bfloat16)
    gate = jnp.dot(mlp_input, gate_weight.T, preferred_element_type=jnp.float32)
    up_part = jnp.dot(mlp_input, up_weight.T, preferred_element_type=jnp.float32)
    hidden = (jax.nn.silu(gate) * up_part).astype(jnp.bfloat16)
    mlp_out = jnp.dot(hidden, down_weight, preferred_element_type=jnp.float32)
    mixed = jnp.einsum('tij,tjc->tic', res_mix, stream_wide, precision=lax.Precision.HIGHEST)
    mixed = mixed + post_gate[:, :, None] * mlp_out[:, None, :]
    return mixed.astype(jnp.bfloat16)
```

```python
import jax
import jax.numpy as jnp
from jax import lax
from jax.sharding import PartitionSpec as P

D = 7168
ITERS = 20
EPSILON = 1e-06
CHUNKS = 2


def flip(value, axis, bits):
    size = lax.axis_size(axis)
    return lax.ppermute(value, axis, [(i, i ^ bits) for i in range(size)])


def normalize(sweep_index, matrix):
    matrix = matrix / jnp.sum(matrix, axis=2, keepdims=True)
    return matrix / jnp.sum(matrix, axis=1, keepdims=True)


def contract_last(weights, rows):
    return lax.dot_general(
        weights, rows, (((1,), (1,)), ((), ())), preferred_element_type=jnp.float32
    )


def gather_tokens(rows):
    size = lax.axis_size("dp")
    bit = size // 2
    while bit > 2:
        rows = jnp.concatenate((rows, flip(rows, "dp", bit)), axis=0)
        bit //= 2
    others = [flip(rows, "dp", k) for k in range(1, 2 * bit)]
    return jnp.concatenate([rows] + others, axis=0)


def scatter_tokens(total):
    size = lax.axis_size("dp")
    near = min(size, 4)
    step = total.shape[0] // near
    sent = total.astype(jnp.bfloat16)
    got = [flip(sent[k * step : (k + 1) * step], "dp", k) for k in range(1, near)]
    kept = total[:step]
    for part in got:
        kept = kept + part.astype(jnp.float32)
    bit = near
    while bit < size:
        half = kept.shape[0] // 2
        part = flip(kept[half:].astype(jnp.bfloat16), "dp", bit)
        kept = kept[:half] + part.astype(jnp.float32)
        bit *= 2
    return kept


def per_device(streams, mix_weight, mix_bias, gate_weight, up_weight, down_weight):
    tok_rows, stream_count, width_local = streams.shape
    logit_count = mix_weight.shape[0]
    flat_rows = streams.reshape(tok_rows, stream_count * width_local)
    flat_weight = mix_weight.reshape(logit_count, stream_count * width_local)
    raw_logits = lax.dot_general(
        flat_rows, flat_weight, (((1,), (1,)), ((), ())), preferred_element_type=jnp.float32
    )
    stream_wide = streams.astype(jnp.float32)
    squares = jnp.sum(stream_wide * stream_wide, axis=(1, 2))
    partial = jnp.concatenate((raw_logits, squares[:, None]), axis=1)
    total = jnp.sum(lax.all_gather(partial, "tensor"), axis=0)
    scale_inv = lax.rsqrt(total[:, logit_count] / (stream_count * D) + EPSILON)
    logits = total[:, :logit_count] * scale_inv[:, None] + mix_bias[None, :]
    pre_gate = jax.nn.sigmoid(logits[:, :stream_count])
    post_gate = 2.0 * jax.nn.sigmoid(logits[:, stream_count : 2 * stream_count])
    matrix = jnp.exp(logits[:, 2 * stream_count :]).reshape(-1, stream_count, stream_count)
    res_mix = lax.fori_loop(0, ITERS, normalize, matrix)
    mlp_input = jnp.einsum(
        "ts,tsc->tc", pre_gate, stream_wide, precision=lax.Precision.HIGHEST
    ).astype(jnp.bfloat16)

    rows = gather_tokens(mlp_input)
    units = gate_weight.shape[0]
    half = units // 2
    gate_part = contract_last(gate_weight, rows)
    up_part = contract_last(up_weight, rows)
    low = lax.axis_index("tensor") % 2
    tensor_size = lax.axis_size("tensor")
    step = half // CHUNKS
    hidden_mine = []
    for chunk in range(CHUNKS):
        mine = low * half + chunk * step
        other = (1 - low) * half + chunk * step
        pick = lambda start: jnp.concatenate(
            (
                lax.dynamic_slice_in_dim(gate_part, start, step, 0),
                lax.dynamic_slice_in_dim(up_part, start, step, 0),
            ),
            axis=0,
        )
        both = pick(mine) + flip(pick(other).astype(jnp.bfloat16), "tensor", 1).astype(jnp.float32)
        bit = 2
        while bit < tensor_size:
            both = both + flip(both.astype(jnp.bfloat16), "tensor", bit).astype(jnp.float32)
            bit *= 2
        hidden_mine.append((jax.nn.silu(both[:step]) * both[step:]).astype(jnp.bfloat16))
    hidden_mine = jnp.concatenate(hidden_mine, axis=0)
    hidden_other = flip(hidden_mine, "tensor", 1)
    first = low == 0
    hidden = jnp.concatenate(
        (
            jnp.where(first, hidden_mine, hidden_other),
            jnp.where(first, hidden_other, hidden_mine),
        ),
        axis=0,
    )
    down_part = lax.dot_general(
        hidden, down_weight, (((0,), (0,)), ((), ())), preferred_element_type=jnp.float32
    )
    mlp_out = scatter_tokens(down_part)
    mixed = jnp.einsum("tij,tjc->tic", res_mix, stream_wide, precision=lax.Precision.HIGHEST)
    mixed = mixed + post_gate[:, :, None] * mlp_out[:, None, :]
    return mixed.astype(jnp.bfloat16)


def solution(mesh):
    in_specs = (
        P("dp", None, "tensor"),
        P(None, None, "tensor"),
        P(),
        P("dp", "tensor"),
        P("dp", "tensor"),
        P("dp", "tensor"),
    )
    out_specs = P("dp", None, "tensor")
    return jax.shard_map(
        per_device, mesh=mesh, in_specs=in_specs, out_specs=out_specs, check_vma=False
    )
```

```python
import functools

import jax
import jax.numpy as jnp
from jax import lax
from jax.experimental import pallas as pl
from jax.experimental.pallas import tpu as pltpu
from jax.sharding import PartitionSpec as P


D = 7168
ITERS = 20
EPSILON = 1e-06
LANES = 128
CHUNKS = 3


F32 = jnp.float32
BF16 = jnp.bfloat16
IN_VMEM = pl.BlockSpec(memory_space=pltpu.VMEM)
IN_HBM = pl.BlockSpec(memory_space=pltpu.HBM)
IN_ANY = pl.BlockSpec(memory_space=pl.ANY)
COPIES = 4


def call(body, outs, specs, aliases=None, limit=8 << 20, flops=0, scratch=()):
    return pl.pallas_call(
        body,
        out_shape=outs,
        in_specs=specs,
        out_specs=jax.tree.map(lambda _: IN_VMEM, outs),
        scratch_shapes=scratch,
        input_output_aliases=aliases or {},
        compiler_params=pltpu.CompilerParams(vmem_limit_bytes=limit),
        cost_estimate=pl.CostEstimate(flops=flops, bytes_accessed=0, transcendentals=0),
    )


def in_hbm(value):
    return pltpu.with_memory_space_constraint(value, pltpu.HBM)


def flip(value, axis, bits):
    size = lax.axis_size(axis)
    return lax.ppermute(value, axis, [(i, i ^ bits) for i in range(size)])


def gather_tokens(rows):
    size = lax.axis_size("dp")
    bit = size // 2
    while bit > 2:
        rows = jnp.concatenate((rows, flip(rows, "dp", bit)), axis=0)
        bit //= 2
    others = [flip(rows, "dp", k) for k in range(1, 2 * bit)]
    return jnp.concatenate([rows] + others, axis=0), rows


def scatter_tokens(kept, got):
    size = lax.axis_size("dp")
    for part in got:
        kept = kept + part.astype(F32)
    bit = 4
    while bit < size:
        half = kept.shape[0] // 2
        part = flip(kept[half:].astype(BF16), "dp", bit)
        kept = kept[:half] + part.astype(F32)
        bit *= 2
    return kept


def nt(rows, weights, precision=None):
    return lax.dot_general(
        rows, weights, (((1,), (1,)), ((), ())), preferred_element_type=F32, precision=precision
    )


def logits_body(streams_hbm, weight_hbm, bias_hbm, out_ref, streams_ref, bias_ref, wide_ref, weight_ref, sems):
    tokens, streams, width = wide_ref.shape
    logits = weight_ref.shape[0]
    pairs = ((streams_hbm, wide_ref), (weight_hbm, weight_ref), (bias_hbm, bias_ref))
    copies = [pltpu.make_async_copy(a, b, sems.at[k]) for k, (a, b) in enumerate(pairs)]
    for copy in copies:
        copy.start()
    copies[0].wait()
    squares = jnp.zeros((tokens, width), F32)
    for s in range(streams):
        rows = wide_ref[:, s, :]
        streams_ref[s] = rows
        wide = rows.astype(F32)
        squares = squares + wide * wide
    out_ref[:, logits : logits + 1] = jnp.sum(squares, axis=1, keepdims=True)
    copies[1].wait()
    total = jnp.zeros((tokens, logits), F32)
    for s in range(streams):
        total = total + nt(streams_ref[s], weight_ref[:, s, :])
    out_ref[:, :logits] = total
    copies[2].wait()


def mix_body(partial_ref, bias_ref, streams_ref, logits_ref, rows_ref):
    streams, tokens, width = streams_ref.shape
    count = bias_ref.shape[1]
    total = jnp.sum(partial_ref[...], axis=0)
    scale = lax.rsqrt(total[:, count : count + 1] / (streams * D) + EPSILON)
    logits = total[:, :count] * scale + bias_ref[...]
    logits_ref[:, :count] = logits
    pre = jax.nn.sigmoid(logits[:, :streams])
    rows = jnp.zeros((tokens, width), F32)
    for s in range(streams):
        rows = rows + pre[:, s : s + 1] * streams_ref[s].astype(F32)
    rows_ref[...] = rows.astype(BF16)


def sinkhorn_body(after_ref, logits_ref, out_ref, *, streams):
    logits = logits_ref[...]
    turned = logits.T
    first = 2 * streams
    rows = [jnp.exp(turned[first + i * streams : first + (i + 1) * streams]) for i in range(streams)]
    for _ in range(ITERS):
        rows = [row / jnp.sum(row, axis=0, keepdims=True) for row in rows]
        columns = functools.reduce(jnp.add, rows)
        rows = [row / columns for row in rows]
    post = 2.0 * jax.nn.sigmoid(turned[streams : 2 * streams])
    spare = jnp.zeros((LANES - streams - streams * streams, turned.shape[1]), F32)
    out_ref[...] = jnp.concatenate([post] + rows + [spare], axis=0).T


def load_body(after_ref, weight_ref, out_ref, sems):
    count = sems.shape[0]
    rows = weight_ref.shape[0] // count
    copies = []
    for k in range(count):
        at = pl.ds(k * rows, rows)
        copies.append(pltpu.make_async_copy(weight_ref.at[at], out_ref.at[at], sems.at[k]))
    for copy in copies:
        copy.start()
    for copy in copies:
        copy.wait()


def load(weight, after):
    copies = 1 if weight.shape[0] % (16 * COPIES) else COPIES
    return call(
        load_body,
        jax.ShapeDtypeStruct(weight.shape, weight.dtype),
        [IN_ANY, IN_HBM],
        flops=int(3e9),
        limit=1 << 20,
        scratch=[pltpu.SemaphoreType.DMA((copies,))],
    )(after, in_hbm(weight))


def expand_body(after_ref, x_ref, gate_ref, up_ref, send_ref, keep_ref, *, start):
    low = lax.axis_index("tensor") % 2
    size = send_ref.shape[2]
    half = gate_ref.shape[0] // 2
    x = x_ref[...]
    for own, out in ((1 - low, send_ref), (low, keep_ref)):
        at = pl.ds(pl.multiple_of(own * half + start, 8), size)
        out[0] = nt(x, gate_ref[at, :]).astype(out.dtype)
        out[1] = nt(x, up_ref[at, :]).astype(out.dtype)


def add_body(keep_ref, got_ref, *refs):
    before, (sum_far, sent_far, sum_near, sent_near) = refs[:-4], refs[-4:]
    tokens = sum_far.shape[1]
    done = sum_near.shape[2] - keep_ref.shape[2]
    total = keep_ref[...] + got_ref[...].astype(F32)
    far, near = total[:, tokens:], total[:, :tokens]
    sum_far[...] = far
    sent_far[...] = far.astype(BF16)
    if done:
        sum_near[:, :, :done] = before[0][...]
        sent_near[:, :, :done] = before[1][...]
    sum_near[:, :, done:] = near
    sent_near[:, :, done:] = near.astype(BF16)


def hidden_body(after_ref, *refs):
    out_ref = refs[-1]
    at = 0
    for sum_ref, got_ref in zip(refs[:-1:2], refs[1:-1:2]):
        size = sum_ref.shape[2]
        gate = sum_ref[0] + got_ref[0].astype(F32)
        up = sum_ref[1] + got_ref[1].astype(F32)
        out_ref[:, at : at + size] = (jax.nn.silu(gate) * up).astype(BF16)
        at += size


def reduce_body(after_ref, mine_ref, other_ref, down_ref, *outs):
    low = lax.axis_index("tensor") % 2
    half = down_ref.shape[0] // 2
    total = None
    for own, rows in ((low, mine_ref), (1 - low, other_ref)):
        at = pl.ds(pl.multiple_of(own * half, 8), half)
        part = jnp.dot(rows[...], down_ref[at, :], preferred_element_type=F32)
        total = part if total is None else total + part
    at = 0
    for out_ref in outs:
        size = out_ref.shape[0]
        out_ref[...] = total[at : at + size].astype(out_ref.dtype)
        at += size


def pieces_of(half):
    if half % (CHUNKS * LANES):
        return [(0, half)]
    size = half // CHUNKS
    return [(k * size, size) for k in range(CHUNKS)]


def layer(streams, mix_weight, mix_bias, gate_weight, up_weight, down_weight):
    tokens, stream_count, width = streams.shape
    count = mix_weight.shape[0]
    shape = jax.ShapeDtypeStruct
    partial, turned, bias = call(
        logits_body,
        (
            shape((tokens, LANES), F32),
            shape((stream_count, tokens, width), BF16),
            shape((1, count), F32),
        ),
        [IN_HBM] * 3,
        scratch=[
            pltpu.VMEM(streams.shape, BF16),
            pltpu.VMEM(mix_weight.shape, BF16),
            pltpu.SemaphoreType.DMA((3,)),
        ],
    )(in_hbm(streams), in_hbm(mix_weight), in_hbm(mix_bias[None, :]))
    gathered = lax.all_gather(partial, "tensor")
    logits, rows = call(
        mix_body,
        (shape((tokens, LANES), F32), shape((tokens, width), BF16)),
        [IN_VMEM] * 3,
    )(gathered, bias, turned)

    gate = load(gate_weight, rows)
    rows, near_rows = gather_tokens(rows)
    up = load(up_weight, near_rows)
    every = rows.shape[0]
    part = every // 2
    tensor_size = lax.axis_size("tensor")
    pieces = pieces_of(gate_weight.shape[0] // 2)

    def across(total, sent):
        bit = 2
        while 2 * bit < tensor_size:
            total = total + flip(sent, "tensor", bit).astype(F32)
            sent = total.astype(BF16)
            bit *= 2
        return total, flip(sent, "tensor", bit)

    far, before = [], ()
    afters = [rows]
    for at, (start, size) in enumerate(pieces):
        send, keep = call(
            functools.partial(expand_body, start=start),
            (shape((2, every, size), BF16), shape((2, every, size), F32)),
            [IN_ANY] + [IN_VMEM] * 3,
            flops=8 * every * size * width,
        )(afters[max(0, at - 1)], rows, gate, up)
        got = flip(send, "tensor", 1)
        far_sum, far_sent, *before = call(
            add_body,
            (
                shape((2, part, size), F32),
                shape((2, part, size), BF16),
                shape((2, part, start + size), F32),
                shape((2, part, start + size), BF16),
            ),
            [IN_VMEM] * (2 + len(before)),
        )(keep, got, *before)
        afters.append(far_sent)
        far.append(across(far_sum, far_sent))
    near = across(*before)
    down = load(down_weight, before[1])

    def outward(pairs, after, outs):
        mine = call(
            hidden_body,
            shape((part, gate_weight.shape[0] // 2), BF16),
            [IN_ANY] + [IN_VMEM] * (2 * len(pairs)),
        )(after, *[x for pair in pairs for x in pair])
        other = flip(mine, "tensor", 1)
        return call(
            reduce_body,
            outs,
            [IN_ANY] + [IN_VMEM] * 3,
            flops=4 * part * gate_weight.shape[0] * width,
        )(after, mine, other, down)

    step = every // 4
    sent = [shape((step, width), BF16)] * 2
    two, three = outward(far, before[1], sent)
    got = [flip(two, "dp", 2), flip(three, "dp", 3)]
    kept, one = outward([near], two, [shape((step, width), F32), sent[0]])
    got.append(flip(one, "dp", 1))
    mlp_out = scatter_tokens(kept, got)
    mixing = call(
        functools.partial(sinkhorn_body, streams=stream_count),
        shape((tokens, LANES), F32),
        [IN_ANY, IN_VMEM],
        flops=int(1e9),
    )(kept, logits)
    post_gate = mixing[:, :stream_count]
    entries = mixing[:, stream_count : stream_count + stream_count**2]
    res_mix = entries.reshape(tokens, stream_count, stream_count)
    mixed = jnp.einsum(
        "tij,tjc->tic", res_mix, streams.astype(F32), precision=lax.Precision.HIGHEST
    )
    mixed = mixed + post_gate[:, :, None] * mlp_out[:, None, :]
    return mixed.astype(BF16)


def solution(mesh):
    in_specs = (
        P("dp", None, "tensor"),
        P(None, None, "tensor"),
        P(),
        P("dp", "tensor"),
        P("dp", "tensor"),
        P("dp", "tensor"),
    )
    out_specs = P("dp", None, "tensor")
    return jax.shard_map(layer, mesh=mesh, in_specs=in_specs, out_specs=out_specs, check_vma=False)
```

```python
import functools

import jax
import jax.numpy as jnp
from jax import lax
from jax.experimental import pallas as pl
from jax.experimental.pallas import tpu as pltpu
from jax.sharding import PartitionSpec as P


D = 7168
ITERS = 20
EPSILON = 1e-06
LANES = 128
CHUNKS = 3


F32 = jnp.float32
BF16 = jnp.bfloat16
IN_VMEM = pl.BlockSpec(memory_space=pltpu.VMEM)
IN_HBM = pl.BlockSpec(memory_space=pltpu.HBM)
IN_ANY = pl.BlockSpec(memory_space=pl.ANY)
COPIES = 4


def call(body, outs, specs, aliases=None, limit=8 << 20, flops=0, scratch=()):
    return pl.pallas_call(
        body,
        out_shape=outs,
        in_specs=specs,
        out_specs=jax.tree.map(lambda _: IN_VMEM, outs),
        scratch_shapes=scratch,
        input_output_aliases=aliases or {},
        compiler_params=pltpu.CompilerParams(vmem_limit_bytes=limit),
        cost_estimate=pl.CostEstimate(flops=flops, bytes_accessed=0, transcendentals=0),
    )


def in_hbm(value):
    return pltpu.with_memory_space_constraint(value, pltpu.HBM)


def flip(value, axis, bits):
    size = lax.axis_size(axis)
    return lax.ppermute(value, axis, [(i, i ^ bits) for i in range(size)])


def gather_tokens(rows):
    size = lax.axis_size("dp")
    bit = size // 2
    while bit > 2:
        rows = jnp.concatenate((rows, flip(rows, "dp", bit)), axis=0)
        bit //= 2
    others = [flip(rows, "dp", k) for k in range(1, 2 * bit)]
    return jnp.concatenate([rows] + others, axis=0), rows


def scatter_tokens(kept, got):
    size = lax.axis_size("dp")
    for part in got:
        kept = kept + part.astype(F32)
    bit = 4
    while bit < size:
        half = kept.shape[0] // 2
        part = flip(kept[half:].astype(BF16), "dp", bit)
        kept = kept[:half] + part.astype(F32)
        bit *= 2
    return kept


def nt(rows, weights, precision=None):
    return lax.dot_general(
        rows, weights, (((1,), (1,)), ((), ())), preferred_element_type=F32, precision=precision
    )


def group(count, streams):
    shape = (count, count * streams)
    row = lax.broadcasted_iota(jnp.int32, shape, 0)
    column = lax.broadcasted_iota(jnp.int32, shape, 1)
    return (column // streams == row).astype(F32)


def logits_body(streams_hbm, weight_hbm, bias_hbm, out_ref, streams_ref, bias_ref, wide_ref, weight_ref, sems):
    tokens, streams, width = wide_ref.shape
    logits = weight_ref.shape[0]
    pairs = ((streams_hbm, wide_ref), (weight_hbm, weight_ref), (bias_hbm, bias_ref))
    copies = [pltpu.make_async_copy(a, b, sems.at[k]) for k, (a, b) in enumerate(pairs)]
    for copy in copies:
        copy.start()
    copies[0].wait()
    for s in range(streams):
        streams_ref[s] = wide_ref[:, s, :]
    rows = wide_ref[...].reshape(tokens * streams, width)
    wide = rows.astype(F32)
    squares = jnp.sum(wide * wide, axis=1, keepdims=True)
    copies[1].wait()
    pairs = nt(rows, weight_ref[...].reshape(logits * streams, width))
    token = lax.broadcasted_iota(jnp.int32, pairs.shape, 0)
    logit = lax.broadcasted_iota(jnp.int32, pairs.shape, 1)
    pairs = jnp.where(token % streams == logit % streams, pairs, 0.0)
    by_token = jnp.dot(
        group(tokens, streams),
        jnp.concatenate([pairs, squares], axis=1),
        preferred_element_type=F32,
        precision=lax.Precision.HIGHEST,
    )
    out_ref[:, :logits] = nt(
        by_token[:, : logits * streams], group(logits, streams), lax.Precision.HIGHEST
    )
    out_ref[:, logits : logits + 1] = by_token[:, logits * streams :]
    copies[2].wait()


def mix_body(bias_ref, streams_ref, *refs):
    *part_refs, logits_ref, rows_ref = refs
    streams, tokens, width = streams_ref.shape
    count = bias_ref.shape[1]
    total = functools.reduce(jnp.add, [ref[...] for ref in part_refs])
    scale = lax.rsqrt(total[:, count : count + 1] / (streams * D) + EPSILON)
    logits = total[:, :count] * scale + bias_ref[...]
    logits_ref[:, :count] = logits
    pre = jax.nn.sigmoid(logits[:, :streams])
    rows = jnp.zeros((tokens, width), F32)
    for s in range(streams):
        rows = rows + pre[:, s : s + 1] * streams_ref[s].astype(F32)
    rows_ref[...] = rows.astype(BF16)


def sinkhorn_body(after_ref, logits_ref, out_ref, *, streams):
    logits = logits_ref[...]
    turned = logits.T
    first = 2 * streams
    rows = [jnp.exp(turned[first + i * streams : first + (i + 1) * streams]) for i in range(streams)]
    for _ in range(ITERS):
        rows = [row / jnp.sum(row, axis=0, keepdims=True) for row in rows]
        columns = functools.reduce(jnp.add, rows)
        rows = [row / columns for row in rows]
    post = 2.0 * jax.nn.sigmoid(turned[streams : 2 * streams])
    spare = jnp.zeros((LANES - streams - streams * streams, turned.shape[1]), F32)
    out_ref[...] = jnp.concatenate([post] + rows + [spare], axis=0).T


def load_body(after_ref, *refs, spans):
    n = len(spans)
    weights, outs, sems = refs[:n], refs[-1 - n : -1], refs[-1]
    copies = []
    for weight, out, (first, last) in zip(weights, outs, spans):
        count = 1 if (last - first) % (16 * COPIES) else COPIES
        rows = (last - first) // count
        for k in range(count):
            at = pl.ds(first + k * rows, rows)
            sem = sems.at[len(copies)]
            copies.append(pltpu.make_async_copy(weight.at[at], out.at[at], sem))
    for copy in copies:
        copy.start()
    for copy in copies:
        copy.wait()


def load(after, *jobs):
    spans = [tuple(weight.shape[0] * x // 6 for x in part) for weight, _, *part in jobs]
    earlier = [e for _, e, *_ in jobs if e is not None]
    aliases, at = {}, 1 + len(jobs)
    for k, (_, e, *_) in enumerate(jobs):
        if e is not None:
            aliases[at] = k
            at += 1
    return call(
        functools.partial(load_body, spans=spans),
        tuple(jax.ShapeDtypeStruct(weight.shape, weight.dtype) for weight, *_ in jobs),
        [IN_ANY] + [IN_HBM] * len(jobs) + [IN_VMEM] * len(earlier),
        flops=int(2e9),
        limit=1 << 20,
        aliases=aliases,
        scratch=[pltpu.SemaphoreType.DMA((COPIES * len(jobs),))],
    )(after, *[in_hbm(weight) for weight, *_ in jobs], *earlier)


def expand_body(after_ref, x_ref, gate_ref, up_ref, send_ref, keep_ref, *, at):
    low = lax.axis_index("tensor") % 2
    size = send_ref.shape[2]
    half = gate_ref.shape[0] // 2
    x = x_ref[...]
    for own, out in ((1 - low, send_ref), (low, keep_ref)):
        units = pl.ds(pl.multiple_of(own * half + at * size, 8), size)
        out[0] = nt(x, gate_ref[units, :]).astype(out.dtype)
        out[1] = nt(x, up_ref[units, :]).astype(out.dtype)


def part_body(keep_ref, got_ref, *refs):
    before, (sum_far, sent_far, sum_near, sent_near) = refs[:-4], refs[-4:]
    tokens = sum_far.shape[1]
    done = sum_near.shape[2] - keep_ref.shape[2]
    total = keep_ref[...] + got_ref[...].astype(F32)
    far, near = total[:, tokens:], total[:, :tokens]
    sum_far[...] = far
    sent_far[...] = far.astype(BF16)
    if done:
        sum_near[:, :, :done] = before[0][...]
        sent_near[:, :, :done] = before[1][...]
    sum_near[:, :, done:] = near
    sent_near[:, :, done:] = near.astype(BF16)


def hidden_body(after_ref, *refs):
    out_ref = refs[-1]
    at = 0
    for sum_ref, got_ref in zip(refs[:-1:2], refs[1:-1:2]):
        size = sum_ref.shape[2]
        gate = sum_ref[0] + got_ref[0].astype(F32)
        up = sum_ref[1] + got_ref[1].astype(F32)
        out_ref[:, at : at + size] = (jax.nn.silu(gate) * up).astype(BF16)
        at += size


def own_body(mine_ref, down_ref, out_ref):
    half = down_ref.shape[0] // 2
    at = pl.ds(pl.multiple_of(lax.axis_index("tensor") % 2 * half, 8), half)
    out_ref[...] = jnp.dot(mine_ref[...], down_ref[at, :], preferred_element_type=F32)


def other_body(own_ref, other_ref, down_ref, *outs):
    half = down_ref.shape[0] // 2
    at = pl.ds(pl.multiple_of((1 - lax.axis_index("tensor") % 2) * half, 8), half)
    total = own_ref[...] + jnp.dot(other_ref[...], down_ref[at, :], preferred_element_type=F32)
    row = 0
    for out_ref in outs:
        size = out_ref.shape[0]
        out_ref[...] = total[row : row + size].astype(out_ref.dtype)
        row += size


def pieces_of(half):
    if half % (CHUNKS * LANES):
        return [(0, half)]
    size = half // CHUNKS
    return [(k * size, size) for k in range(CHUNKS)]


def layer(streams, mix_weight, mix_bias, gate_weight, up_weight, down_weight):
    tokens, stream_count, width = streams.shape
    count = mix_weight.shape[0]
    shape = jax.ShapeDtypeStruct
    partial, turned, bias = call(
        logits_body,
        (
            shape((tokens, LANES), F32),
            shape((stream_count, tokens, width), BF16),
            shape((1, count), F32),
        ),
        [IN_HBM] * 3,
        scratch=[
            pltpu.VMEM(streams.shape, BF16),
            pltpu.VMEM(mix_weight.shape, BF16),
            pltpu.SemaphoreType.DMA((3,)),
        ],
    )(in_hbm(streams), in_hbm(mix_weight), in_hbm(mix_bias[None, :]))
    parts = [partial] + [flip(partial, "tensor", k) for k in range(1, lax.axis_size("tensor"))]
    (gate,) = load(partial, (gate_weight, None, 0, 2))
    logits, rows = call(
        mix_body,
        (shape((tokens, LANES), F32), shape((tokens, width), BF16)),
        [IN_VMEM] * (2 + len(parts)),
    )(bias, turned, *parts)

    (gate,) = load(rows, (gate_weight, gate, 2, 6))
    rows, near_rows = gather_tokens(rows)
    up, down = load(near_rows, (up_weight, None, 0, 6), (down_weight, None, 0, 2))
    every = rows.shape[0]
    part = every // 2
    tensor_size = lax.axis_size("tensor")
    pieces = pieces_of(gate_weight.shape[0] // 2)

    def across(total, sent):
        bit = 2
        while 2 * bit < tensor_size:
            total = total + flip(sent, "tensor", bit).astype(F32)
            sent = total.astype(BF16)
            bit *= 2
        return total, flip(sent, "tensor", bit)

    far, before = [], ()
    after = rows
    for at, (start, size) in enumerate(pieces):
        send, keep = call(
            functools.partial(expand_body, at=at),
            (shape((2, every, size), BF16), shape((2, every, size), F32)),
            [IN_ANY] + [IN_VMEM] * 3,
            flops=8 * every * size * width,
        )(after, rows, gate, up)
        got = flip(send, "tensor", 1)
        after = send
        far_sum, far_sent, *before = call(
            part_body,
            (
                shape((2, part, size), F32),
                shape((2, part, size), BF16),
                shape((2, part, start + size), F32),
                shape((2, part, start + size), BF16),
            ),
            [IN_VMEM] * (2 + len(before)),
        )(keep, got, *before)
        far.append(across(far_sum, far_sent))
    near = [across(*before)]
    (down,) = load(before[1], (down_weight, down, 2, 6))
    half = gate_weight.shape[0] // 2

    def outward(pairs, after, outs):
        mine = call(
            hidden_body,
            shape((part, half), BF16),
            [IN_ANY] + [IN_VMEM] * (2 * len(pairs)),
        )(after, *[x for pair in pairs for x in pair])
        other = flip(mine, "tensor", 1)
        flops = 2 * part * half * width
        own = call(own_body, shape((part, width), F32), [IN_VMEM] * 2, flops=flops)(mine, down)
        return call(other_body, outs, [IN_VMEM] * 3, flops=flops)(own, other, down)

    step = every // 4
    sent = shape((step, width), BF16)
    two, three = outward(far, before[1], [sent, sent])
    got = [flip(two, "dp", 2), flip(three, "dp", 3)]
    kept, one = outward(near, two, [shape((step, width), F32), sent])
    got.append(flip(one, "dp", 1))
    mixing = call(
        functools.partial(sinkhorn_body, streams=stream_count),
        shape((tokens, LANES), F32),
        [IN_ANY, IN_VMEM],
        flops=int(1e9),
    )(one, logits)
    post_gate = mixing[:, :stream_count]
    entries = mixing[:, stream_count : stream_count + stream_count**2]
    res_mix = entries.reshape(tokens, stream_count, stream_count)
    mixed = jnp.einsum(
        "tij,tjc->tic", res_mix, streams.astype(F32), precision=lax.Precision.HIGHEST
    )
    mixed, post_gate = lax.optimization_barrier((mixed, post_gate))
    mlp_out = scatter_tokens(kept, got)
    mixed = mixed + post_gate[:, :, None] * mlp_out[:, None, :]
    return mixed.astype(BF16)


def solution(mesh):
    in_specs = (
        P("dp", None, "tensor"),
        P(None, None, "tensor"),
        P(),
        P("dp", "tensor"),
        P("dp", "tensor"),
        P("dp", "tensor"),
    )
    out_specs = P("dp", None, "tensor")
    return jax.shard_map(layer, mesh=mesh, in_specs=in_specs, out_specs=out_specs, check_vma=False)
```

```python
import functools

import jax
import jax.numpy as jnp
from jax import lax
from jax.experimental import pallas as pl
from jax.experimental.pallas import tpu as pltpu
from jax.sharding import PartitionSpec as P


D = 7168
ITERS = 20
EPSILON = 1e-06
LANES = 128


F32 = jnp.float32
BF16 = jnp.bfloat16
IN_VMEM = pl.BlockSpec(memory_space=pltpu.VMEM)
IN_HBM = pl.BlockSpec(memory_space=pltpu.HBM)
IN_ANY = pl.BlockSpec(memory_space=pl.ANY)
COPIES = 2


def call(body, outs, specs, aliases=None, limit=8 << 20, flops=0, scratch=()):
    return pl.pallas_call(
        body,
        out_shape=outs,
        in_specs=specs,
        out_specs=jax.tree.map(lambda _: IN_VMEM, outs),
        scratch_shapes=scratch,
        input_output_aliases=aliases or {},
        compiler_params=pltpu.CompilerParams(vmem_limit_bytes=limit),
        cost_estimate=pl.CostEstimate(flops=flops, bytes_accessed=0, transcendentals=0),
    )


def in_hbm(value):
    return pltpu.with_memory_space_constraint(value, pltpu.HBM)


def flip(value, axis, bits):
    size = lax.axis_size(axis)
    return lax.ppermute(value, axis, [(i, i ^ bits) for i in range(size)])


def gather_tokens(rows):
    size = lax.axis_size("dp")
    bit = size // 2
    while bit > 2:
        rows = jnp.concatenate((rows, flip(rows, "dp", bit)), axis=0)
        bit //= 2
    others = []
    for k in range(1, 2 * bit):
        others.append(flip(rows, "dp", k))
    return jnp.concatenate([rows] + others, axis=0), rows


def scatter_tokens(kept, bit):
    while bit < lax.axis_size("dp"):
        half = kept.shape[0] // 2
        part = flip(kept[half:].astype(BF16), "dp", bit)
        kept = kept[:half] + part.astype(F32)
        bit *= 2
    return kept


def nt(rows, weights, precision=None):
    return lax.dot_general(
        rows, weights, (((1,), (1,)), ((), ())), preferred_element_type=F32, precision=precision
    )


def group(count, streams):
    shape = (count, count * streams)
    row = lax.broadcasted_iota(jnp.int32, shape, 0)
    column = lax.broadcasted_iota(jnp.int32, shape, 1)
    return (column // streams == row).astype(F32)


def logits_body(streams_hbm, weight_hbm, bias_hbm, out_ref, wide_ref, bias_ref, weight_ref, sems):
    tokens, streams, width = wide_ref.shape
    logits = weight_ref.shape[0]
    pairs = ((streams_hbm, wide_ref), (weight_hbm, weight_ref), (bias_hbm, bias_ref))
    copies = [pltpu.make_async_copy(a, b, sems.at[k]) for k, (a, b) in enumerate(pairs)]
    for copy in copies:
        copy.start()
    copies[0].wait()
    rows = wide_ref[...].reshape(tokens * streams, width)
    wide = rows.astype(F32)
    squares = jnp.sum(wide * wide, axis=1, keepdims=True)
    copies[1].wait()
    pairs = nt(rows, weight_ref[...].reshape(logits * streams, width))
    token = lax.broadcasted_iota(jnp.int32, pairs.shape, 0)
    logit = lax.broadcasted_iota(jnp.int32, pairs.shape, 1)
    pairs = jnp.where(token % streams == logit % streams, pairs, 0.0)
    by_token = jnp.dot(
        group(tokens, streams),
        jnp.concatenate([pairs, squares], axis=1),
        preferred_element_type=F32,
        precision=lax.Precision.HIGHEST,
    )
    out_ref[:, :logits] = nt(
        by_token[:, : logits * streams], group(logits, streams), lax.Precision.HIGHEST
    )
    out_ref[:, logits : logits + 1] = by_token[:, logits * streams :]
    copies[2].wait()


def turn_body(wide_ref, streams_ref):
    for s in range(streams_ref.shape[0]):
        streams_ref[s] = wide_ref[:, s, :]


def mix_body(bias_ref, streams_ref, *refs):
    *part_refs, logits_ref, rows_ref = refs
    streams, tokens, width = streams_ref.shape
    count = bias_ref.shape[1]
    total = functools.reduce(jnp.add, [ref[...] for ref in part_refs])
    scale = lax.rsqrt(total[:, count : count + 1] / (streams * D) + EPSILON)
    logits = total[:, :count] * scale + bias_ref[...]
    logits_ref[:, :count] = logits
    pre = jax.nn.sigmoid(logits[:, :streams])
    rows = jnp.zeros((tokens, width), F32)
    for s in range(streams):
        rows = rows + pre[:, s : s + 1] * streams_ref[s].astype(F32)
    rows_ref[...] = rows.astype(BF16)


def sinkhorn_body(after_ref, logits_ref, out_ref, *, streams):
    logits = logits_ref[...]
    turned = logits.T
    first = 2 * streams
    rows = [jnp.exp(turned[first + i * streams : first + (i + 1) * streams]) for i in range(streams)]
    for _ in range(ITERS):
        rows = [row / jnp.sum(row, axis=0, keepdims=True) for row in rows]
        columns = functools.reduce(jnp.add, rows)
        rows = [row / columns for row in rows]
    post = 2.0 * jax.nn.sigmoid(turned[streams : 2 * streams])
    spare = jnp.zeros((LANES - streams - streams * streams, turned.shape[1]), F32)
    out_ref[...] = jnp.concatenate([post] + rows + [spare], axis=0).T


def copies_of(weights, outs, spans, sems):
    copies = []
    for weight, out, parts in zip(weights, outs, spans):
        for first, last in parts:
            count = 1 if (last - first) % (16 * COPIES) else COPIES
            rows = (last - first) // count
            for k in range(count):
                at = pl.ds(first + k * rows, rows)
                sem = sems.at[len(copies)]
                copies.append(pltpu.make_async_copy(weight.at[at], out.at[at], sem))
    return copies


def start_now(copies):
    @pl.when(lax.axis_index("tensor") >= 0)
    def _():
        for copy in copies:
            copy.start()


def load_body(after_ref, *refs, spans):
    n = len(spans)
    copies = copies_of(refs[:n], refs[-1 - n : -1], spans, refs[-1])
    for copy in copies:
        copy.start()
    for copy in copies:
        copy.wait()


def sems_for(spans):
    return pltpu.SemaphoreType.DMA((COPIES * sum(len(parts) for parts in spans),))


def load(after, *jobs):
    spans = [parts for *_, parts in jobs]
    earlier = [e for _, e, _ in jobs if e is not None]
    aliases, at = {}, 1 + len(jobs)
    for k, (_, e, _) in enumerate(jobs):
        if e is not None:
            aliases[at] = k
            at += 1
    return call(
        functools.partial(load_body, spans=spans),
        tuple(jax.ShapeDtypeStruct(weight.shape, weight.dtype) for weight, *_ in jobs),
        [IN_ANY] + [IN_HBM] * len(jobs) + [IN_VMEM] * len(earlier),
        flops=int(2e9),
        limit=1 << 20,
        aliases=aliases,
        scratch=[sems_for(spans)],
    )(after, *[in_hbm(weight) for weight, *_ in jobs], *earlier)


def expand_body(after_ref, x_ref, gate_ref, up_ref, *refs, start, spans):
    copies = []
    if spans:
        gate_hbm, up_hbm, send_ref, keep_ref, gate_out, up_out, sems = refs
        copies = copies_of((gate_hbm, up_hbm), (gate_out, up_out), (spans, spans), sems)
        start_now(copies)
    else:
        send_ref, keep_ref = refs
    low = lax.axis_index("tensor") % 2
    size = send_ref.shape[2]
    half = gate_ref.shape[0] // 2
    x = x_ref[...]
    for own, out in ((1 - low, send_ref), (low, keep_ref)):
        units = pl.ds(pl.multiple_of(own * half + start, 8), size)
        out[0] = nt(x, gate_ref[units, :]).astype(out.dtype)
        out[1] = nt(x, up_ref[units, :]).astype(out.dtype)
    for copy in copies:
        copy.wait()


def part_body(keep_ref, got_ref, *refs):
    before, (sum_far, sent_far, sum_near, sent_near) = refs[:-4], refs[-4:]
    tokens = sum_far.shape[1]
    done = sum_near.shape[2] - keep_ref.shape[2]
    total = keep_ref[...] + got_ref[...].astype(F32)
    far, near = total[:, tokens:], total[:, :tokens]
    sum_far[...] = far
    sent_far[...] = far.astype(BF16)
    if done:
        sum_near[:, :, :done] = before[0][...]
        sent_near[:, :, :done] = before[1][...]
    sum_near[:, :, done:] = near
    sent_near[:, :, done:] = near.astype(BF16)


def hidden_body(after_ref, *refs):
    out_ref = refs[-1]
    at = 0
    for sum_ref, got_ref in zip(refs[:-1:2], refs[1:-1:2]):
        size = sum_ref.shape[2]
        gate = sum_ref[0] + got_ref[0].astype(F32)
        up = sum_ref[1] + got_ref[1].astype(F32)
        out_ref[:, at : at + size] = (jax.nn.silu(gate) * up).astype(BF16)
        at += size


def own_body(mine_ref, down_ref, out_ref):
    half = down_ref.shape[0] // 2
    at = pl.ds(pl.multiple_of(lax.axis_index("tensor") % 2 * half, 8), half)
    out_ref[...] = jnp.dot(mine_ref[...], down_ref[at, :], preferred_element_type=F32)


def other_body(own_ref, other_ref, down_ref, *outs):
    half = down_ref.shape[0] // 2
    at = pl.ds(pl.multiple_of((1 - lax.axis_index("tensor") % 2) * half, 8), half)
    total = own_ref[...] + jnp.dot(other_ref[...], down_ref[at, :], preferred_element_type=F32)
    row = 0
    for out_ref in outs:
        size = out_ref.shape[0]
        out_ref[...] = total[row : row + size].astype(out_ref.dtype)
        row += size


def pool_body(kept_ref, two_ref, three_ref, *outs):
    total = kept_ref[...] + two_ref[...].astype(F32) + three_ref[...].astype(F32)
    row = 0
    for out_ref in outs:
        size = out_ref.shape[0]
        out_ref[...] = total[row : row + size].astype(out_ref.dtype)
        row += size


def pieces_of(half):
    if half % LANES or half < 3 * LANES:
        return [(0, half)]
    tiles = half // LANES
    last = max(1, 2 * tiles // 9)
    middle = max(1, tiles // 3)
    sizes = [x * LANES for x in (tiles - last - middle, middle, last)]
    return [(sum(sizes[:k]), size) for k, size in enumerate(sizes)]


def layer(streams, mix_weight, mix_bias, gate_weight, up_weight, down_weight):
    tokens, stream_count, width = streams.shape
    count = mix_weight.shape[0]
    shape = jax.ShapeDtypeStruct
    partial, local, bias = call(
        logits_body,
        (
            shape((tokens, LANES), F32),
            shape(streams.shape, BF16),
            shape((1, count), F32),
        ),
        [IN_HBM] * 3,
        scratch=[
            pltpu.VMEM(mix_weight.shape, BF16),
            pltpu.SemaphoreType.DMA((3,)),
        ],
    )(in_hbm(streams), in_hbm(mix_weight), in_hbm(mix_bias[None, :]))
    parts = [partial]
    for k in range(1, lax.axis_size("tensor")):
        parts.append(flip(partial, "tensor", k))
    turned = call(turn_body, shape((stream_count, tokens, width), BF16), [IN_VMEM])(local)
    logits, rows = call(
        mix_body,
        (shape((tokens, LANES), F32), shape((tokens, width), BF16)),
        [IN_VMEM] * (2 + len(parts)),
    )(bias, turned, *parts)

    half = gate_weight.shape[0] // 2
    pieces = pieces_of(half)
    late = pieces[-1][1] if len(pieces) > 1 else 0
    soon = half - late
    (gate,) = load(rows, (gate_weight, None, [(0, soon), (half, half + soon - late)]))
    rows, near_rows = gather_tokens(rows)
    jobs = [(up_weight, None, [(0, soon), (half, half + soon)])]
    if late:
        jobs.append((gate_weight, gate, [(half + soon - late, half + soon)]))
    up, *more = load(near_rows, *jobs)
    gate = more[0] if late else gate
    every = rows.shape[0]
    part = every // 2
    tensor_size = lax.axis_size("tensor")

    def across(total, sent):
        bit = 2
        while 2 * bit < tensor_size:
            total = total + flip(sent, "tensor", bit).astype(F32)
            sent = total.astype(BF16)
            bit *= 2
        return total, flip(sent, "tensor", bit)

    far, before = [], ()
    after = rows
    for at, (start, size) in enumerate(pieces):
        outs = [shape((2, every, size), BF16), shape((2, every, size), F32)]
        spans = [(soon, half), (half + soon, 2 * half)] if late and not at else []
        held = shape(gate_weight.shape, BF16)
        send, keep, *more = call(
            functools.partial(expand_body, start=start, spans=spans),
            outs + ([held, held] if spans else []),
            [IN_ANY] + [IN_VMEM] * 3 + ([IN_HBM] * 2 if spans else []),
            aliases={2: 2, 3: 3} if spans else {},
            flops=8 * every * size * width,
            scratch=[sems_for((spans, spans))] if spans else [],
        )(after, rows, gate, up, *([in_hbm(gate_weight), in_hbm(up_weight)] if spans else []))
        if spans:
            gate, up = more
        got = flip(send, "tensor", 1)
        after = send
        far_sum, far_sent, *before = call(
            part_body,
            (
                shape((2, part, size), F32),
                shape((2, part, size), BF16),
                shape((2, part, start + size), F32),
                shape((2, part, start + size), BF16),
            ),
            [IN_VMEM] * (2 + len(before)),
        )(keep, got, *before)
        far.append(across(far_sum, far_sent))
    near = [across(*before)]
    (down,) = load(before[1], (down_weight, None, [(0, 2 * half)]))

    def outward(pairs, after, outs):
        mine = call(
            hidden_body,
            shape((part, half), BF16),
            [IN_ANY] + [IN_VMEM] * (2 * len(pairs)),
        )(after, *[x for pair in pairs for x in pair])
        other = flip(mine, "tensor", 1)
        flops = 2 * part * half * width
        own = call(own_body, shape((part, width), F32), [IN_VMEM] * 2, flops=flops)(mine, down)
        return call(other_body, outs, [IN_VMEM] * 3, flops=flops)(own, other, down)

    step = every // 4
    sent = shape((step, width), BF16)
    two, three = outward(far, before[1], [sent, sent])
    got = [flip(two, "dp", 2), flip(three, "dp", 3)]
    cut = step // 2 if lax.axis_size("dp") > 4 else step
    kept, *ones = outward(
        near, two, [shape((step, width), F32)] + [shape((cut, width), BF16)] * (step // cut)
    )
    direct = []
    for k, one in enumerate(ones):
        direct.append(flip(one, "dp", 1 + 4 * k))
    mlp_out, *rest = call(
        pool_body,
        [shape((cut, width), F32)] + [shape((cut, width), BF16)] * (step // cut - 1),
        [IN_VMEM] * (1 + len(got)),
    )(kept, *got)
    direct += [flip(part_sum, "dp", 4) for part_sum in rest]
    mixing = call(
        functools.partial(sinkhorn_body, streams=stream_count),
        shape((tokens, LANES), F32),
        [IN_ANY, IN_VMEM],
        flops=int(1e9),
    )((rest or ones)[0], logits)
    post_gate = mixing[:, :stream_count]
    entries = mixing[:, stream_count : stream_count + stream_count**2]
    res_mix = entries.reshape(tokens, stream_count, stream_count)
    mixed = jnp.einsum(
        "tij,tjc->tic", res_mix, streams.astype(F32), precision=lax.Precision.HIGHEST
    )
    mixed, post_gate = lax.optimization_barrier((mixed, post_gate))
    for part_sum in direct:
        mlp_out = mlp_out + part_sum.astype(F32)
    mlp_out = scatter_tokens(mlp_out, 8)
    mixed = mixed + post_gate[:, :, None] * mlp_out[:, None, :]
    return mixed.astype(BF16)


def solution(mesh):
    in_specs = (
        P("dp", None, "tensor"),
        P(None, None, "tensor"),
        P(),
        P("dp", "tensor"),
        P("dp", "tensor"),
        P("dp", "tensor"),
    )
    out_specs = P("dp", None, "tensor")
    return jax.shard_map(layer, mesh=mesh, in_specs=in_specs, out_specs=out_specs, check_vma=False)
```

```python
import functools

import jax
import jax.numpy as jnp
from jax import lax
from jax.experimental import pallas as pl
from jax.experimental.pallas import tpu as pltpu
from jax.sharding import PartitionSpec as P


D = 7168
ITERS = 20
EPSILON = 1e-06
LANES = 128


F32 = jnp.float32
BF16 = jnp.bfloat16
IN_VMEM = pl.BlockSpec(memory_space=pltpu.VMEM)
IN_HBM = pl.BlockSpec(memory_space=pltpu.HBM)
IN_ANY = pl.BlockSpec(memory_space=pl.ANY)
COPIES = 2


def call(body, outs, specs, aliases=None, limit=8 << 20, flops=0, scratch=()):
    return pl.pallas_call(
        body,
        out_shape=outs,
        in_specs=specs,
        out_specs=jax.tree.map(lambda _: IN_VMEM, outs),
        scratch_shapes=scratch,
        input_output_aliases=aliases or {},
        compiler_params=pltpu.CompilerParams(vmem_limit_bytes=limit),
        cost_estimate=pl.CostEstimate(flops=flops, bytes_accessed=0, transcendentals=0),
    )


def in_hbm(value):
    return pltpu.with_memory_space_constraint(value, pltpu.HBM)


def flip(value, axis, bits):
    size = lax.axis_size(axis)
    return lax.ppermute(value, axis, [(i, i ^ bits) for i in range(size)])


def gather_tokens(rows):
    size = lax.axis_size("dp")
    bit = size // 2
    while bit > 2:
        rows = jnp.concatenate((rows, flip(rows, "dp", bit)), axis=0)
        bit //= 2
    others = []
    for k in range(1, 2 * bit):
        others.append(flip(rows, "dp", k))
    return jnp.concatenate([rows] + others, axis=0), rows


def scatter_tokens(kept, bit):
    while bit < lax.axis_size("dp"):
        half = kept.shape[0] // 2
        part = flip(kept[half:].astype(BF16), "dp", bit)
        kept = kept[:half] + part.astype(F32)
        bit *= 2
    return kept


def nt(rows, weights, precision=None):
    return lax.dot_general(
        rows, weights, (((1,), (1,)), ((), ())), preferred_element_type=F32, precision=precision
    )


def group(count, streams):
    shape = (count, count * streams)
    row = lax.broadcasted_iota(jnp.int32, shape, 0)
    column = lax.broadcasted_iota(jnp.int32, shape, 1)
    return (column // streams == row).astype(F32)


def logits_body(streams_hbm, weight_hbm, bias_hbm, out_ref, wide_ref, bias_ref, weight_ref, sems):
    tokens, streams, width = wide_ref.shape
    logits = weight_ref.shape[0]
    pairs = ((streams_hbm, wide_ref), (weight_hbm, weight_ref), (bias_hbm, bias_ref))
    copies = [pltpu.make_async_copy(a, b, sems.at[k]) for k, (a, b) in enumerate(pairs)]
    for copy in copies:
        copy.start()
    copies[0].wait()
    rows = wide_ref[...].reshape(tokens * streams, width)
    wide = rows.astype(F32)
    squares = jnp.sum(wide * wide, axis=1, keepdims=True)
    copies[1].wait()
    pairs = nt(rows, weight_ref[...].reshape(logits * streams, width))
    token = lax.broadcasted_iota(jnp.int32, pairs.shape, 0)
    logit = lax.broadcasted_iota(jnp.int32, pairs.shape, 1)
    pairs = jnp.where(token % streams == logit % streams, pairs, 0.0)
    both = jnp.concatenate([pairs, squares], axis=1)
    by_token = jnp.sum(both.reshape(tokens, streams, both.shape[1]), axis=1)
    out_ref[:, :logits] = nt(
        by_token[:, : logits * streams], group(logits, streams), lax.Precision.HIGHEST
    )
    out_ref[:, logits : logits + 1] = by_token[:, logits * streams :]
    copies[2].wait()


def turn_body(wide_ref, streams_ref):
    for s in range(streams_ref.shape[0]):
        streams_ref[s] = wide_ref[:, s, :]


def mix_body(bias_ref, streams_ref, *refs):
    *part_refs, logits_ref, rows_ref = refs
    streams, tokens, width = streams_ref.shape
    count = bias_ref.shape[1]
    total = functools.reduce(jnp.add, [ref[...] for ref in part_refs])
    scale = lax.rsqrt(total[:, count : count + 1] / (streams * D) + EPSILON)
    logits = total[:, :count] * scale + bias_ref[...]
    logits_ref[:, :count] = logits
    pre = jax.nn.sigmoid(logits[:, :streams])
    rows = jnp.zeros((tokens, width), F32)
    for s in range(streams):
        rows = rows + pre[:, s : s + 1] * streams_ref[s].astype(F32)
    rows_ref[...] = rows.astype(BF16)


def sinkhorn_body(after_ref, logits_ref, out_ref, *, streams):
    logits = logits_ref[...]
    turned = logits.T
    first = 2 * streams
    rows = [jnp.exp(turned[first + i * streams : first + (i + 1) * streams]) for i in range(streams)]
    for _ in range(ITERS):
        rows = [row / jnp.sum(row, axis=0, keepdims=True) for row in rows]
        columns = functools.reduce(jnp.add, rows)
        rows = [row / columns for row in rows]
    post = 2.0 * jax.nn.sigmoid(turned[streams : 2 * streams])
    spare = jnp.zeros((LANES - streams - streams * streams, turned.shape[1]), F32)
    out_ref[...] = jnp.concatenate([post] + rows + [spare], axis=0).T


def copies_of(weights, outs, spans, sems):
    copies = []
    for weight, out, parts in zip(weights, outs, spans):
        for first, last in parts:
            count = 1 if (last - first) % (16 * COPIES) else COPIES
            rows = (last - first) // count
            for k in range(count):
                at = pl.ds(first + k * rows, rows)
                sem = sems.at[len(copies)]
                copies.append(pltpu.make_async_copy(weight.at[at], out.at[at], sem))
    return copies


def start_now(copies):
    @pl.when(lax.axis_index("tensor") >= 0)
    def _():
        for copy in copies:
            copy.start()


def load_body(after_ref, *refs, spans):
    n = len(spans)
    copies = copies_of(refs[:n], refs[-1 - n : -1], spans, refs[-1])
    for copy in copies:
        copy.start()
    for copy in copies:
        copy.wait()


def sems_for(spans):
    return pltpu.SemaphoreType.DMA((COPIES * sum(len(parts) for parts in spans),))


def load(after, *jobs):
    spans = [parts for *_, parts in jobs]
    earlier = [e for _, e, _ in jobs if e is not None]
    aliases, at = {}, 1 + len(jobs)
    for k, (_, e, _) in enumerate(jobs):
        if e is not None:
            aliases[at] = k
            at += 1
    return call(
        functools.partial(load_body, spans=spans),
        tuple(jax.ShapeDtypeStruct(weight.shape, weight.dtype) for weight, *_ in jobs),
        [IN_ANY] + [IN_HBM] * len(jobs) + [IN_VMEM] * len(earlier),
        flops=int(2e9),
        limit=1 << 20,
        aliases=aliases,
        scratch=[sems_for(spans)],
    )(after, *[in_hbm(weight) for weight, *_ in jobs], *earlier)


def expand_body(after_ref, x_ref, gate_ref, up_ref, *refs, start, spans):
    copies = []
    if spans:
        gate_hbm, up_hbm, send_ref, keep_ref, gate_out, up_out, sems = refs
        copies = copies_of((gate_hbm, up_hbm), (gate_out, up_out), (spans, spans), sems)
        start_now(copies)
    else:
        send_ref, keep_ref = refs
    low = lax.axis_index("tensor") % 2
    size = send_ref.shape[2]
    half = gate_ref.shape[0] // 2
    x = x_ref[...]
    for own, out in ((1 - low, send_ref), (low, keep_ref)):
        units = pl.ds(pl.multiple_of(own * half + start, 8), size)
        out[0] = nt(x, gate_ref[units, :]).astype(out.dtype)
        out[1] = nt(x, up_ref[units, :]).astype(out.dtype)
    for copy in copies:
        copy.wait()


def part_body(keep_ref, got_ref, *refs):
    before, (sum_far, sent_far, sum_near, sent_near) = refs[:-4], refs[-4:]
    tokens = sum_far.shape[1]
    done = sum_near.shape[2] - keep_ref.shape[2]
    total = keep_ref[...] + got_ref[...].astype(F32)
    far, near = total[:, tokens:], total[:, :tokens]
    sum_far[...] = far
    sent_far[...] = far.astype(BF16)
    if done:
        sum_near[:, :, :done] = before[0][...]
        sent_near[:, :, :done] = before[1][...]
    sum_near[:, :, done:] = near
    sent_near[:, :, done:] = near.astype(BF16)


def hidden_body(after_ref, *refs):
    out_ref = refs[-1]
    at = 0
    for sum_ref, got_ref in zip(refs[:-1:2], refs[1:-1:2]):
        size = sum_ref.shape[2]
        gate = sum_ref[0] + got_ref[0].astype(F32)
        up = sum_ref[1] + got_ref[1].astype(F32)
        out_ref[:, at : at + size] = (jax.nn.silu(gate) * up).astype(BF16)
        at += size


def own_body(mine_ref, down_ref, out_ref):
    half = down_ref.shape[0] // 2
    at = pl.ds(pl.multiple_of(lax.axis_index("tensor") % 2 * half, 8), half)
    out_ref[...] = jnp.dot(mine_ref[...], down_ref[at, :], preferred_element_type=F32)


def other_body(own_ref, other_ref, down_ref, *outs):
    half = down_ref.shape[0] // 2
    at = pl.ds(pl.multiple_of((1 - lax.axis_index("tensor") % 2) * half, 8), half)
    total = own_ref[...] + jnp.dot(other_ref[...], down_ref[at, :], preferred_element_type=F32)
    row = 0
    for out_ref in outs:
        size = out_ref.shape[0]
        out_ref[...] = total[row : row + size].astype(out_ref.dtype)
        row += size


def pool_body(kept_ref, two_ref, three_ref, *outs):
    total = kept_ref[...] + two_ref[...].astype(F32) + three_ref[...].astype(F32)
    row = 0
    for out_ref in outs:
        size = out_ref.shape[0]
        out_ref[...] = total[row : row + size].astype(out_ref.dtype)
        row += size


def pieces_of(half):
    if half % LANES or half < 3 * LANES:
        return [(0, half)]
    tiles = half // LANES
    last = max(1, 2 * tiles // 9)
    middle = max(1, tiles // 3)
    sizes = [x * LANES for x in (tiles - last - middle, middle, last)]
    return [(sum(sizes[:k]), size) for k, size in enumerate(sizes)]


def layer(streams, mix_weight, mix_bias, gate_weight, up_weight, down_weight):
    tokens, stream_count, width = streams.shape
    count = mix_weight.shape[0]
    shape = jax.ShapeDtypeStruct
    partial, local, bias = call(
        logits_body,
        (
            shape((tokens, LANES), F32),
            shape(streams.shape, BF16),
            shape((1, count), F32),
        ),
        [IN_HBM] * 3,
        scratch=[
            pltpu.VMEM(mix_weight.shape, BF16),
            pltpu.SemaphoreType.DMA((3,)),
        ],
    )(in_hbm(streams), in_hbm(mix_weight), in_hbm(mix_bias[None, :]))
    parts = [partial]
    for k in range(1, lax.axis_size("tensor")):
        parts.append(flip(partial, "tensor", k))
    turned = call(turn_body, shape((stream_count, tokens, width), BF16), [IN_VMEM])(local)
    logits, rows = call(
        mix_body,
        (shape((tokens, LANES), F32), shape((tokens, width), BF16)),
        [IN_VMEM] * (2 + len(parts)),
    )(bias, turned, *parts)

    half = gate_weight.shape[0] // 2
    pieces = pieces_of(half)
    late = pieces[-1][1] if len(pieces) > 1 else 0
    soon = half - late
    (gate,) = load(rows, (gate_weight, None, [(0, soon), (half, half + soon - late)]))
    rows, near_rows = gather_tokens(rows)
    jobs = [(up_weight, None, [(0, soon), (half, half + soon)])]
    if late:
        jobs.append((gate_weight, gate, [(half + soon - late, half + soon)]))
    up, *more = load(near_rows, *jobs)
    gate = more[0] if late else gate
    every = rows.shape[0]
    part = every // 2
    tensor_size = lax.axis_size("tensor")

    def across(total, sent):
        bit = 2
        while 2 * bit < tensor_size:
            total = total + flip(sent, "tensor", bit).astype(F32)
            sent = total.astype(BF16)
            bit *= 2
        return total, flip(sent, "tensor", bit)

    far, before = [], ()
    after = rows
    for at, (start, size) in enumerate(pieces):
        outs = [shape((2, every, size), BF16), shape((2, every, size), F32)]
        spans = [(soon, half), (half + soon, 2 * half)] if late and not at else []
        held = shape(gate_weight.shape, BF16)
        send, keep, *more = call(
            functools.partial(expand_body, start=start, spans=spans),
            outs + ([held, held] if spans else []),
            [IN_ANY] + [IN_VMEM] * 3 + ([IN_HBM] * 2 if spans else []),
            aliases={2: 2, 3: 3} if spans else {},
            flops=8 * every * size * width,
            scratch=[sems_for((spans, spans))] if spans else [],
        )(after, rows, gate, up, *([in_hbm(gate_weight), in_hbm(up_weight)] if spans else []))
        if spans:
            gate, up = more
        got = flip(send, "tensor", 1)
        after = send
        far_sum, far_sent, *before = call(
            part_body,
            (
                shape((2, part, size), F32),
                shape((2, part, size), BF16),
                shape((2, part, start + size), F32),
                shape((2, part, start + size), BF16),
            ),
            [IN_VMEM] * (2 + len(before)),
        )(keep, got, *before)
        far.append(across(far_sum, far_sent))
    near = [across(*before)]
    (down,) = load(before[1], (down_weight, None, [(0, 2 * half)]))

    def outward(pairs, after, outs):
        mine = call(
            hidden_body,
            shape((part, half), BF16),
            [IN_ANY] + [IN_VMEM] * (2 * len(pairs)),
        )(after, *[x for pair in pairs for x in pair])
        other = flip(mine, "tensor", 1)
        flops = 2 * part * half * width
        own = call(own_body, shape((part, width), F32), [IN_VMEM] * 2, flops=flops)(mine, down)
        return call(other_body, outs, [IN_VMEM] * 3, flops=flops)(own, other, down)

    step = every // 4
    sent = shape((step, width), BF16)
    two, three = outward(far, before[1], [sent, sent])
    got = [flip(two, "dp", 2), flip(three, "dp", 3)]
    cut = step // 2 if lax.axis_size("dp") > 4 else step
    kept, *ones = outward(
        near, two, [shape((step, width), F32)] + [shape((cut, width), BF16)] * (step // cut)
    )
    direct = []
    for k, one in enumerate(ones):
        direct.append(flip(one, "dp", 1 + 4 * k))
    mlp_out, *rest = call(
        pool_body,
        [shape((cut, width), F32)] + [shape((cut, width), BF16)] * (step // cut - 1),
        [IN_VMEM] * (1 + len(got)),
    )(kept, *got)
    direct += [flip(part_sum, "dp", 4) for part_sum in rest]
    mixing = call(
        functools.partial(sinkhorn_body, streams=stream_count),
        shape((tokens, LANES), F32),
        [IN_ANY, IN_VMEM],
        flops=int(1e9),
    )((rest or ones)[0], logits)
    post_gate = mixing[:, :stream_count]
    entries = mixing[:, stream_count : stream_count + stream_count**2]
    res_mix = entries.reshape(tokens, stream_count, stream_count)
    mixed = jnp.einsum(
        "tij,tjc->tic", res_mix, streams.astype(F32), precision=lax.Precision.HIGHEST
    )
    mixed, post_gate = lax.optimization_barrier((mixed, post_gate))
    for part_sum in direct:
        mlp_out = mlp_out + part_sum.astype(F32)
    mlp_out = scatter_tokens(mlp_out, 8)
    mixed = mixed + post_gate[:, :, None] * mlp_out[:, None, :]
    return mixed.astype(BF16)


def solution(mesh):
    in_specs = (
        P("dp", None, "tensor"),
        P(None, None, "tensor"),
        P(),
        P("dp", "tensor"),
        P("dp", "tensor"),
        P("dp", "tensor"),
    )
    out_specs = P("dp", None, "tensor")
    return jax.shard_map(layer, mesh=mesh, in_specs=in_specs, out_specs=out_specs, check_vma=False)
```
